32 devices in a mesh: section: 8 (over z, x), expert: 4 (over y, core).
Axes of the slice: x: 2, y: 2, z: 4, core: 2. Of those that a mesh axis runs over, the one named last changes fastest.
Arguments:
- tokens: bfloat16 [16, 32, 768], P(None, 'expert'), may hold values from -6 to 6
- route_ids: int32 [8, 16, 32, 2], P('section'), may hold values from 0 to 3, all different within a row; in each aligned block of 8 rows (0 to 7, 8 to 15, ..., all dimensions but the last counted through in order) at most 8 rows name the same one
- router: bfloat16 [8, 768, 4], P('section'), may hold values from -0.21875 to 0.21875
- norm_gain: float32 [8, 768], P('section'), may hold values from 0.1 to 1.9
- weight_in: bfloat16 [8, 4, 768, 3072], P('section', 'expert'), may hold values from -0.21875 to 0.21875
- weight_out: bfloat16 [8, 4, 3072, 768], P('section', 'expert'), may hold values from -0.109375 to 0.109375
Outputs:
- layer_states: bfloat16 [8, 16, 32, 768], P('section', None, 'expert')
The draws below stay inside these ranges and needn't reach their ends.
Inputs may be any that keep to these rules, and one draw needn't show every extreme that they name: `route_ids`: each row names two different experts. In each aligned block of 8 rows (the tokens of one micro-batch on one index of the expert axis) no expert is named by more than 8 rows, and in some blocks one expert is named by exactly 8.
All inputs are finite; a program needn't handle non-finite values.
Results may differ from the reference program's by a relative error of at most 0.028.
Values may be sent and summed in bfloat16 or wider, within the bound.
No kernel may reach another device: no remote copies, remote signals or barrier semaphores. Data moves between devices by JAX's collectives and lax.ppermute only.
A program may use at most 64 MiB of HBM per device.

```python
import math
import jax
import jax.numpy as jnp
import numpy as np
from jax import lax

D = 768
FF = 3072
TOK_MB = 8
MICRO = 16
EXPERTS = 4
LAYERS = 8
TOKENS_MB = 32
CAP = 8
N_EXPERT = 4


def block_levels(own_key, extent, cuts, smallest, largest):
    def one(dim, shards_of):
        steps = jax.random.uniform(jax.random.fold_in(jax.random.fold_in(own_key, 6), dim), (shards_of,), jnp.float32, smallest / len(cuts), largest / len(cuts))
        return jnp.repeat(jnp.exp(steps), extent[dim] // shards_of).reshape((-1,) + (1,) * (len(extent) - dim - 1))

    loudness = one(*cuts[0])
    for cut in cuts[1:]:
        loudness = loudness * one(*cut)
    return loudness


def deal_out(own_key, own, number, rows, number_of, top, reach, lean):
    order = jax.random.permutation(own_key, number_of)
    packed, common = shares(number_of, rows * top, reach, lean, True), shares(number_of, rows * top, reach, lean, False)
    places = jnp.arange(number_of)

    def named(tallies, turn):
        used = int((tallies > 0).sum())
        fixed = max(1, used // 4)
        passed = fixed + (places - fixed + turn * (used - fixed)) % max(1, number_of - fixed)
        return jnp.zeros((number_of,), jnp.int32).at[order[jnp.where(places < fixed, places, passed)]].set(jnp.asarray(tallies, jnp.int32))

    tallies = jnp.where(number % 4 == 0, named(packed, number // 4), named(common, number - number // 4 - 1))
    mixed = jax.random.permutation(jax.random.fold_in(own, 3), number_of)
    source_of, receiver = mixed[0:number_of // 2 * 2:2], mixed[1:number_of // 2 * 2:2]
    margin = jnp.minimum(tallies[source_of] - 1, reach - tallies[receiver]) // 2
    margin = jnp.where((source_of == order[0]) | (receiver == order[0]) | (tallies[receiver] == 0), 0, jnp.maximum(margin, 0))
    passed = jax.random.randint(jax.random.fold_in(own, 4), (number_of // 2,), 0, 1 << 20) % (margin + 1)
    tallies = tallies.at[source_of].add(-passed).at[receiver].add(passed)
    items = jnp.searchsorted(jnp.cumsum(tallies), jnp.arange(rows * top), side="right").astype(jnp.int32)
    listing = items.reshape(top, rows).T
    listing = listing[jax.random.permutation(jax.random.fold_in(own, 1), rows)]
    turn = jax.random.randint(jax.random.fold_in(own, 2), (rows, 1), 0, top)
    return jnp.take_along_axis(listing, (jnp.arange(top)[None, :] + turn) % top, axis=1)


def shares(count, total, limit, slope, full):
    loads = [(1 << 20) // math.isqrt(grade ** slope) + 1 for grade in range(1, count + 1)]
    largest = limit if full else min(limit, max(-(-total // count), total * loads[0] // sum(loads)))
    least = 1 if total - largest >= count - 1 else 0
    counts, spare = [largest] + [least] * (count - 1), total - largest - least * (count - 1)
    while spare > 0:
        free = [i for i in range(1, count) if counts[i] < largest] or [i for i in range(1, count) if counts[i] < limit]
        mass, budget = sum([loads[i] for i in free]), spare
        for i in free:
            addition = min(limit - counts[i], max(1, budget * loads[i] // mass), spare)
            counts[i] = counts[i] + addition
            spare = spare - addition
    return np.array(counts)


def centred(rng, shape, spread, most, cuts=(), kind=jnp.bfloat16):
    array = jax.random.normal(rng, shape, jnp.float32) * spread
    if len(cuts) > 0:
        array = block_levels(rng, shape, cuts, -0.22, 0.18) * array
    return jnp.clip(array, min=-most, max=most).astype(kind)


def setup_inputs(seed: int = 0) -> dict:
    streams_of = jax.random.split(jax.random.key(seed), 7)
    tokens = centred(streams_of[0], (MICRO, TOKENS_MB, D), 1.0, 6.0, ((1, 4),))
    route_ids_keys = jax.random.split(jax.random.fold_in(streams_of[1], 1), LAYERS * MICRO * TOKENS_MB // TOK_MB)
    route_ids_turns = jax.random.permutation(jax.random.fold_in(streams_of[1], 3), LAYERS * MICRO * TOKENS_MB // TOK_MB)
    route_ids = jax.vmap(lambda own, number: deal_out(jax.random.fold_in(streams_of[1], 2), own, number, TOK_MB, EXPERTS, 2, CAP, 2))(route_ids_keys, route_ids_turns).reshape((LAYERS, MICRO, TOKENS_MB, 2))
    router = centred(streams_of[2], (LAYERS, D, EXPERTS), D ** -0.5, 0.21875, ((0, 8),))
    norm_gain = jnp.clip(1.0 + 0.18 * jax.random.normal(streams_of[3], (LAYERS, D), jnp.float32), 0.1, 1.9)
    weight_in = centred(streams_of[4], (LAYERS, EXPERTS, D, FF), D ** -0.5, 0.21875, ((0, 8), (1, 4)))
    weight_out = centred(streams_of[5], (LAYERS, EXPERTS, FF, D), FF ** -0.5, 0.109375, ((0, 8), (1, 4)))
    return {"tokens": tokens, "route_ids": route_ids, "router": router, "norm_gain": norm_gain, "weight_in": weight_in, "weight_out": weight_out}


epsilon = 1e-06

def run_expert(item):
    rows_in, first_matrix, second_matrix = item
    hidden = jax.nn.relu(jnp.dot(rows_in, first_matrix, preferred_element_type=jnp.float32)).astype(jnp.bfloat16)
    return jnp.dot(hidden, second_matrix, preferred_element_type=jnp.float32).astype(jnp.bfloat16)

def reference(tokens, route_ids, router, norm_gain, weight_in, weight_out):
    owners = N_EXPERT

    def one_layer(carried, layer_args):
        routes, router_block, gain_row, expert_in, expert_out = layer_args
        stream = carried.astype(jnp.float32)
        inverse = lax.rsqrt(lax.optimization_barrier(jnp.mean(stream * stream, axis=-1, keepdims=True)) + epsilon)
        normed = (stream * inverse * gain_row).astype(jnp.bfloat16)
        logits = jnp.einsum('mtd,de->mte', normed.astype(jnp.float32), router_block.astype(jnp.float32))
        gate_values = jax.nn.sigmoid(jnp.take_along_axis(logits, routes, axis=2))
        blocks = routes.reshape(MICRO, owners, TOK_MB * 2)
        onehot = (blocks[..., None] == jnp.arange(EXPERTS, dtype=jnp.int32)).astype(jnp.int32)
        earlier = jnp.cumsum(onehot, axis=2) - onehot
        position = lax.optimization_barrier(jnp.sum(onehot * earlier, axis=3))
        block_index = jnp.arange(MICRO * owners, dtype=jnp.int32).reshape(MICRO, owners, 1)
        slot_row = (block_index * CAP + position).reshape(-1).astype(jnp.int32)
        chosen = blocks.reshape(-1).astype(jnp.int32)
        source = jnp.repeat(normed.reshape(-1, D), 2, axis=0)
        buffer = jnp.zeros((EXPERTS, MICRO * owners * CAP, D), jnp.bfloat16).at[chosen, slot_row].set(source)
        produced = lax.map(run_expert, (buffer, expert_in, expert_out))
        picked = produced[chosen, slot_row].astype(jnp.float32).reshape(MICRO, TOKENS_MB, 2, D)
        mixed = stream + gate_values[..., 0:1] * picked[:, :, 0] + gate_values[..., 1:2] * picked[:, :, 1]
        result = mixed.astype(jnp.bfloat16)
        return (result, result)
    leftover, states = lax.scan(one_layer, tokens, (route_ids, router, norm_gain, weight_in, weight_out))
    return states
```

```python
import functools

import jax
import jax.numpy as jnp
from jax import lax
from jax.experimental import pallas as pl
from jax.experimental.pallas import tpu as pltpu
from jax.sharding import PartitionSpec as P

epsilon = 1e-06
CHUNKS = 2
LANES = 128
UNROLLED = 32


def expert_kernel(
    tile, mine_ref, other_ref, mask_ref, gain_ref, router_ref, in_ref, out_ref,
    send_ref, keep_ref, in_tiles, out_tiles, normed, gate, total, sems,
):
    steps = in_tiles.shape[0]
    half = mine_ref.shape[0]
    block = min(2 * half, 256)

    def copies(i):
        start = pl.multiple_of(i * tile, tile)
        return (
            pltpu.make_async_copy(in_ref.at[:, pl.ds(start, tile)], in_tiles.at[i], sems.at[0, i]),
            pltpu.make_async_copy(out_ref.at[pl.ds(start, tile), :], out_tiles.at[i], sems.at[1, i]),
        )

    for i in range(steps):
        for copy in copies(i):
            copy.start()
    for place, ref in ((0, mine_ref), (half, other_ref)):

        def normalize(g, carry):
            source = pl.ds(pl.multiple_of(g * (block // 2), block // 2), block // 2)
            stream = ref[source, :].astype(jnp.float32)
            inverse = lax.rsqrt(jnp.mean(stream * stream, axis=-1, keepdims=True) + epsilon)
            value = (stream * inverse * gain_ref[...]).astype(jnp.bfloat16)
            rows = pl.ds(pl.multiple_of(place + g * (block // 2), block // 2), block // 2)
            normed[rows, :] = value
            logits = jnp.dot(value, router_ref[...], preferred_element_type=jnp.float32)
            gate[rows, :] = jax.nn.sigmoid(logits) * mask_ref[rows, :]
            total[rows, :] = jnp.zeros((block // 2, total.shape[1]), jnp.float32)
            return carry

        lax.fori_loop(0, 2 * half // block, normalize, 0)

    def step(i, carry):
        for copy in copies(i):
            copy.wait()

        def group(g, carry):
            rows = pl.ds(pl.multiple_of(g * block, block), block)
            hidden = jnp.dot(normed[rows, :], in_tiles[i], preferred_element_type=jnp.float32)
            hidden = jnp.maximum(hidden, 0.0).astype(jnp.bfloat16)
            total[rows, :] += jnp.dot(hidden, out_tiles[i], preferred_element_type=jnp.float32)
            return carry

        return lax.fori_loop(0, 2 * half // block, group, carry)

    lax.fori_loop(0, steps, step, 0)
    for place, ref in ((0, send_ref), (half, keep_ref)):

        def finish(g, carry):
            rows = pl.ds(pl.multiple_of(place + g * (block // 2), block // 2), block // 2)
            target = pl.ds(pl.multiple_of(g * (block // 2), block // 2), block // 2)
            for column in range(0, total.shape[1], LANES):
                lanes = pl.ds(column, LANES)
                ref[target, lanes] = (total[rows, lanes] * gate[rows, :]).astype(ref.dtype)
            return carry

        lax.fori_loop(0, 2 * half // block, finish, 0)


def run_expert(mine, other, mask, gain, router, weight_in, weight_out):
    half, features = mine.shape
    hidden_total = weight_in.shape[1]
    tile = 512
    steps = hidden_total // tile
    rows = 2 * half
    vmem, anywhere = pltpu.VMEM, pl.ANY
    return pl.pallas_call(
        functools.partial(expert_kernel, tile),
        out_shape=(jax.ShapeDtypeStruct(mine.shape, jnp.bfloat16),) * 2,
        in_specs=[pl.BlockSpec(memory_space=vmem)] * 5 + [pl.BlockSpec(memory_space=anywhere)] * 2,
        out_specs=(pl.BlockSpec(memory_space=vmem),) * 2,
        scratch_shapes=[
            pltpu.VMEM((steps, features, tile), jnp.bfloat16),
            pltpu.VMEM((steps, tile, features), jnp.bfloat16),
            pltpu.VMEM((rows, features), jnp.bfloat16),
            pltpu.VMEM((rows, LANES), jnp.float32),
            pltpu.VMEM((rows, features), jnp.float32),
            pltpu.SemaphoreType.DMA((2, steps)),
        ],
        compiler_params=pltpu.CompilerParams(vmem_limit_bytes=40 * 2**20),
        cost_estimate=pl.CostEstimate(
            flops=4 * rows * features * hidden_total,
            bytes_accessed=4 * features * hidden_total,
            transcendentals=0,
        ),
    )(mine, other, mask, gain, router, weight_in, weight_out)


def body(tokens, route_ids, router, norm_gain, weight_in, weight_out):
    sections, experts = lax.axis_size("section"), lax.axis_size("expert")
    section, member = lax.axis_index("section"), lax.axis_index("expert")
    chip, core = member // 2, member % 2
    chips = experts // 2
    micro_count, tok_rows, features = tokens.shape
    part = micro_count // CHUNKS
    rows = part * tok_rows
    gain = norm_gain.astype(jnp.float32)
    expert_in, expert_out = weight_in[0, 0], weight_out[0, 0]
    column = lax.dynamic_slice_in_dim(router[0], member, 1, axis=1)
    column = jnp.broadcast_to(column, (features, LANES))

    named = jnp.any(route_ids[0] == member, axis=-1).reshape(CHUNKS, part, chips, 2, tok_rows)
    named = named.transpose(0, 3, 2, 1, 4)
    named = jnp.where(core == 0, named[:, ::-1], named).astype(jnp.float32)
    masks = jnp.broadcast_to(named.reshape(CHUNKS, -1, 1), (CHUNKS, experts * rows, LANES))

    def place(s, e):
        return s * experts + e

    def across(value, other_of):
        pairs = [
            (place(s, e), place(*other_of(s, e))) for s in range(sections) for e in range(experts)
        ]
        return lax.ppermute(value, ("section", "expert"), pairs)

    def paired(s, odd):
        other = s - 1 if (s % 2 == 0) == odd else s + 1
        return other if 0 <= other < sections else s

    def to_paired(value, odd, flip):
        def other_of(s, e):
            other = paired(s, odd)
            return (other, e ^ (flip if other != s else (flip or 1)))

        return across(value, other_of)

    def swapped(value):
        return across(value, lambda s, e: (s, e ^ 1))

    def own_of(other):
        return lax.dynamic_slice_in_dim(other, chip * rows, rows, axis=0)

    mine, others = [], []
    for j in range(CHUNKS):
        entering = lax.all_gather(tokens[j * part : (j + 1) * part].reshape(rows, features), "expert")
        entering = entering.reshape(chips, 2, rows, features)
        mine.append(lax.dynamic_index_in_dim(entering, 1 - core, 1, False).reshape(-1, features))
        others.append(lax.dynamic_index_in_dim(entering, core, 1, False).reshape(-1, features))
    saved = [jnp.zeros((rows, features), jnp.bfloat16) for _ in range(CHUNKS)]

    def turn_of(turn, odd, state):
        mine, others, saved = (list(part_state) for part_state in state)
        for j in range(CHUNKS):
            saved[j] = jnp.where(section == turn, own_of(others[j]), saved[j])
            send, keep = run_expert(
                mine[j], others[j], masks[j], gain, column, expert_in, expert_out
            )
            stream = jnp.where(chip == 0, others[j], jnp.zeros_like(others[j]))
            partial = keep.astype(jnp.float32) + swapped(send).astype(jnp.float32)
            partial = (partial + stream.astype(jnp.float32)).astype(jnp.bfloat16)
            arrived = [to_paired(partial, odd, 2 * k + 1) for k in range(chips)]
            mine[j] = sum(a.astype(jnp.float32) for a in arrived).astype(jnp.bfloat16)
            others[j] = swapped(mine[j])
        return mine, others, saved

    def two_turns(pair, state):
        return turn_of(2 * pair + 1, True, turn_of(2 * pair, False, state))

    state = (mine, others, saved)
    if sections * chips <= UNROLLED:
        for pair in range(sections // 2):
            state = two_turns(pair, state)
    else:
        state = lax.fori_loop(0, sections // 2, two_turns, state)
    mine, others, saved = state
    whole = jnp.concatenate(saved, axis=0)
    from_even, from_odd = to_paired(whole, False, 0), to_paired(whole, True, 0)
    returned = jnp.where(section % 2 == 0, from_even, from_odd)
    last = jnp.concatenate([own_of(other) for other in others], axis=0)
    states = jnp.where(section == sections - 1, last, returned)
    return states.reshape(1, micro_count, tok_rows, features)


def solution(mesh):
    placed = (
        P(None, "expert", None),
        P("section", None, None, None),
        P("section", None, None),
        P("section", None),
        P("section", "expert", None, None),
        P("section", "expert", None, None),
    )
    return jax.shard_map(
        body,
        mesh=mesh,
        in_specs=placed,
        out_specs=P("section", None, "expert", None),
        check_vma=False,
    )
```

```python
import jax
import jax.numpy as jnp
from jax import lax
from jax.experimental import pallas as pl
from jax.experimental.pallas import tpu as pltpu
from jax.sharding import PartitionSpec as P

epsilon = 1e-06
STREAMS = 2
GROUPS = 2
LANES = 128
UNROLLED = 32


def expert_kernel(
    mine_ref, other_ref, mask_ref, gain_ref, router_ref, in_ref, out_ref, behind_ref,
    send_ref, keep_ref,
):
    half, features = mine_ref.shape
    block = min(half, 64)

    def group(g, carry):
        rows = pl.ds(pl.multiple_of(g * block, block), block)
        lower = pl.ds(pl.multiple_of(half + g * block, block), block)

        def normed_of(ref):
            stream = ref[rows, :].astype(jnp.float32)
            inverse = lax.rsqrt(jnp.mean(stream * stream, axis=-1, keepdims=True) + epsilon)
            return (stream * inverse * gain_ref[...]).astype(jnp.bfloat16)

        normed = jnp.concatenate([normed_of(mine_ref), normed_of(other_ref)], axis=0)
        logits = jnp.dot(normed, router_ref[...], preferred_element_type=jnp.float32)
        mask = jnp.concatenate([mask_ref[rows, :], mask_ref[lower, :]], axis=0)
        gate = jax.nn.sigmoid(logits) * mask
        hidden = jnp.dot(normed, in_ref[...], preferred_element_type=jnp.float32)
        hidden = jnp.maximum(hidden, 0.0).astype(jnp.bfloat16)
        total = jnp.dot(hidden, out_ref[...], preferred_element_type=jnp.float32)
        for column in range(0, features, LANES):
            lanes = slice(column, column + LANES)
            gated = (total[:, lanes] * gate).astype(send_ref.dtype)
            send_ref[rows, lanes] = gated[:block]
            keep_ref[rows, lanes] = gated[block:]
        return carry

    if half == block:
        group(0, 0)
    else:
        lax.fori_loop(0, half // block, group, 0)


def run_expert(mine, other, mask, gain, router, weight_in, weight_out, behind):
    half, features = mine.shape
    hidden_total = weight_in.shape[1]
    local = pl.BlockSpec(memory_space=pltpu.VMEM)
    return pl.pallas_call(
        expert_kernel,
        out_shape=(jax.ShapeDtypeStruct(mine.shape, jnp.bfloat16),) * 2,
        in_specs=[local] * 7 + [pl.BlockSpec(memory_space=pl.ANY)],
        out_specs=(local,) * 2,
        compiler_params=pltpu.CompilerParams(vmem_limit_bytes=20 * 2**20),
        cost_estimate=pl.CostEstimate(
            flops=8 * half * features * hidden_total,
            bytes_accessed=4 * features * hidden_total,
            transcendentals=0,
        ),
    )(mine, other, mask, gain, router, weight_in, weight_out, behind)


def body(tokens, route_ids, router, norm_gain, weight_in, weight_out):
    sections, experts = lax.axis_size("section"), lax.axis_size("expert")
    section, member = lax.axis_index("section"), lax.axis_index("expert")
    chip, core = member // 2, member % 2
    chips = experts // 2
    micro_count, tok_rows, features = tokens.shape
    pieces = STREAMS * GROUPS
    part = micro_count // pieces
    rows = part * tok_rows
    gain = norm_gain.astype(jnp.float32)
    expert_in, expert_out = weight_in[0, 0], weight_out[0, 0]
    column = lax.dynamic_slice_in_dim(router[0], member, 1, axis=1)
    column = jnp.broadcast_to(column, (features, LANES))

    named = jnp.any(route_ids[0] == member, axis=-1)
    named = named.reshape(GROUPS, STREAMS, part, chips, 2, tok_rows).transpose(1, 0, 4, 3, 2, 5)
    named = jnp.where(core == 0, named[:, :, ::-1], named).astype(jnp.float32)
    masks = named.reshape(STREAMS, GROUPS, experts * rows, 1)
    masks = jnp.broadcast_to(masks, masks.shape[:3] + (LANES,))

    def place(s, e):
        return s * experts + e

    def across(value, other_of):
        pairs = [
            (place(s, e), place(*other_of(s, e))) for s in range(sections) for e in range(experts)
        ]
        return lax.ppermute(value, ("section", "expert"), pairs)

    def to_paired(value, odd, flip):
        def other_of(s, e):
            other = s - 1 if (s % 2 == 0) == odd else s + 1
            if 0 <= other < sections:
                return (other, e ^ flip)
            return (s, e ^ (flip or 1))

        return across(value, other_of)

    def swapped(value):
        return across(value, lambda s, e: (s, e ^ 1))

    def own_of(other):
        return lax.dynamic_slice_in_dim(other, chip * rows, rows, axis=0)

    entering = lax.all_gather(tokens.reshape(-1, features), "expert")
    entering = entering.reshape(chips, 2, GROUPS, STREAMS, rows, features)
    to_mine = lax.dynamic_index_in_dim(entering, 1 - core, 1, False)
    to_other = lax.dynamic_index_in_dim(entering, core, 1, False)

    def piece(source, i, q):
        return source[:, i, q].reshape(-1, features)

    mine = [piece(to_mine, 0, q) for q in range(STREAMS)]
    others = [piece(to_other, 0, q) for q in range(STREAMS)]
    blank = jnp.zeros((rows, features), jnp.bfloat16)
    saved = [[blank] * GROUPS for _ in range(STREAMS)]
    final = [[blank] * GROUPS for _ in range(STREAMS)]
    turns = sections + 2 * (GROUPS - 1)

    def one_turn(turn, odd, state):
        mine, others, saved, final, behind = state
        mine, others = list(mine), list(others)
        saved, final = [list(x) for x in saved], [list(x) for x in final]
        for q in range(STREAMS):
            if not odd:
                for i in range(1, GROUPS):
                    fresh = jnp.logical_and(section == 0, turn == 2 * i)
                    mine[q] = jnp.where(fresh, piece(to_mine, i, q), mine[q])
                    others[q] = jnp.where(fresh, piece(to_other, i, q), others[q])
            own = own_of(others[q])
            for i in range(GROUPS):
                here = section == turn - 2 * i
                saved[q][i] = jnp.where(here, own, saved[q][i])
            index = jnp.clip((turn - section) // 2, 0, GROUPS - 1)
            mask = lax.dynamic_index_in_dim(masks[q], index, 0, False)
            send, keep = run_expert(
                mine[q], others[q], mask, gain, column, expert_in, expert_out, behind
            )
            stream = jnp.where(chip == 0, others[q], jnp.zeros_like(others[q]))
            partial = keep.astype(jnp.float32) + swapped(send).astype(jnp.float32)
            behind = (partial + stream.astype(jnp.float32)).astype(jnp.bfloat16)
            arrived = [to_paired(behind, odd, 2 * k + 1) for k in range(chips)]
            mine[q] = sum(a.astype(jnp.float32) for a in arrived).astype(jnp.bfloat16)
            others[q] = swapped(mine[q])
            for i in range(GROUPS):
                ended = turn == sections - 1 + 2 * i
                final[q][i] = jnp.where(ended, own_of(others[q]), final[q][i])
        return mine, others, saved, final, behind

    def two_turns(pair, state):
        return one_turn(2 * pair + 1, True, one_turn(2 * pair, False, state))

    state = (mine, others, saved, final, mine[0])
    if sections * chips <= UNROLLED:
        for pair in range(turns // 2):
            state = two_turns(pair, state)
    else:
        state = lax.fori_loop(0, turns // 2, two_turns, state)
    saved, final = state[2], state[3]

    def whole(values):
        return jnp.stack([values[q][i] for i in range(GROUPS) for q in range(STREAMS)])

    passed = whole(saved).reshape(-1, features)
    from_even, from_odd = to_paired(passed, False, 0), to_paired(passed, True, 0)
    returned = jnp.where(section % 2 == 0, from_even, from_odd)
    states = jnp.where(section == sections - 1, whole(final).reshape(-1, features), returned)
    return states.reshape(1, micro_count, tok_rows, features)


def solution(mesh):
    placed = (
        P(None, "expert", None),
        P("section", None, None, None),
        P("section", None, None),
        P("section", None),
        P("section", "expert", None, None),
        P("section", "expert", None, None),
    )
    return jax.shard_map(
        body,
        mesh=mesh,
        in_specs=placed,
        out_specs=P("section", None, "expert", None),
        check_vma=False,
    )
```

```python
import jax
import jax.numpy as jnp
from jax import lax
from jax.experimental import pallas as pl
from jax.experimental.pallas import tpu as pltpu
from jax.sharding import PartitionSpec as P


epsilon = 1e-06
STREAMS = 2
GROUPS = 2
LANES = 128
UNROLLED = 32


def expert_kernel(
    mine_ref, other_ref, mask_ref, gain_ref, router_ref, in_ref, out_ref, behind_ref,
    send_ref, keep_ref,
):
    half, features = mine_ref.shape
    block = min(half, 64)

    def group(g, carry):
        rows = pl.ds(pl.multiple_of(g * block, block), block)
        lower = pl.ds(pl.multiple_of(half + g * block, block), block)

        def normed_of(ref):
            stream = ref[rows, :].astype(jnp.float32)
            inverse = lax.rsqrt(jnp.mean(stream * stream, axis=-1, keepdims=True) + epsilon)
            return (stream * inverse * gain_ref[...]).astype(jnp.bfloat16)

        normed = jnp.concatenate([normed_of(mine_ref), normed_of(other_ref)], axis=0)
        logits = jnp.dot(normed, router_ref[...], preferred_element_type=jnp.float32)
        mask = jnp.concatenate([mask_ref[rows, :], mask_ref[lower, :]], axis=0)
        gate = jax.nn.sigmoid(logits) * mask
        hidden = jnp.dot(normed, in_ref[...], preferred_element_type=jnp.float32)
        hidden = jnp.maximum(hidden, 0.0).astype(jnp.bfloat16)
        total = jnp.dot(hidden, out_ref[...], preferred_element_type=jnp.float32)
        for column in range(0, features, LANES):
            lanes = slice(column, column + LANES)
            gated = (total[:, lanes] * gate).astype(send_ref.dtype)
            send_ref[rows, lanes] = gated[:block]
            keep_ref[rows, lanes] = gated[block:]
        return carry

    if half == block:
        group(0, 0)
    else:
        lax.fori_loop(0, half // block, group, 0)


def run_expert(mine, other, mask, gain, router, weight_in, weight_out, behind):
    half, features = mine.shape
    hidden_total = weight_in.shape[1]
    local = pl.BlockSpec(memory_space=pltpu.VMEM)
    return pl.pallas_call(
        expert_kernel,
        out_shape=(jax.ShapeDtypeStruct(mine.shape, jnp.bfloat16),) * 2,
        in_specs=[local] * 7 + [pl.BlockSpec(memory_space=pl.ANY)],
        out_specs=(local,) * 2,
        compiler_params=pltpu.CompilerParams(vmem_limit_bytes=20 * 2**20),
        cost_estimate=pl.CostEstimate(
            flops=8 * half * features * hidden_total,
            bytes_accessed=4 * features * hidden_total,
            transcendentals=0,
        ),
    )(mine, other, mask, gain, router, weight_in, weight_out, behind)


def body(tokens, route_ids, router, norm_gain, weight_in, weight_out):
    sections, experts = lax.axis_size("section"), lax.axis_size("expert")
    section, member = lax.axis_index("section"), lax.axis_index("expert")
    chip, core = member // 2, member % 2
    chips = experts // 2
    micro_count, tok_rows, features = tokens.shape
    pieces = STREAMS * GROUPS
    part = micro_count // pieces
    rows = part * tok_rows
    gain = norm_gain.astype(jnp.float32)
    expert_in, expert_out = weight_in[0, 0], weight_out[0, 0]
    column = lax.dynamic_slice_in_dim(router[0], member, 1, axis=1)
    column = jnp.broadcast_to(column, (features, LANES))

    named = jnp.any(route_ids[0] == member, axis=-1)
    named = named.reshape(GROUPS, STREAMS, part, chips, 2, tok_rows).transpose(1, 0, 4, 3, 2, 5)
    named = jnp.where(core == 0, named[:, :, ::-1], named).astype(jnp.float32)
    masks = named.reshape(STREAMS, GROUPS, experts * rows, 1)
    masks = jnp.broadcast_to(masks, masks.shape[:3] + (LANES,))

    def place(s, e):
        return s * experts + e

    def across(value, other_of):
        pairs = [
            (place(s, e), place(*other_of(s, e))) for s in range(sections) for e in range(experts)
        ]
        return lax.ppermute(value, ("section", "expert"), pairs)

    def to_paired(value, odd, flip):
        def other_of(s, e):
            other = s - 1 if (s % 2 == 0) == odd else s + 1
            if 0 <= other < sections:
                return (other, e ^ flip)
            return (s, e ^ (flip or 1))

        return across(value, other_of)

    def swapped(value):
        return across(value, lambda s, e: (s, e ^ 1))

    def gathered(value):
        count = value.shape[0] // rows
        came = [across(value, lambda s, e, k=k: (s, e ^ (2 * k + 1))) for k in range(chips)]
        came = [v.reshape(count, rows, features) for v in came]
        by_chip = []
        for y in range(chips):
            wanted = came[0]
            for k in range(1, chips):
                wanted = jnp.where(chip ^ y == k, came[k], wanted)
            by_chip.append(wanted)
        return jnp.stack(by_chip, axis=1).reshape(count, -1, features)

    own_tokens = tokens.reshape(-1, features)
    first, later = gathered(own_tokens[:rows]), gathered(own_tokens[rows:])
    entering = [first[0]] + [later[n] for n in range(pieces - 1)]
    turns = sections + 2 * (GROUPS - 1)
    facts = {
        "at": [section == turn for turn in range(turns)],
        "index": [
            jnp.clip((turn - section) // 2, 0, GROUPS - 1).astype(jnp.int32)
            for turn in range(turns)
        ],
        "start": [(chip ^ k) * rows for k in range(chips)],
        "lead": chip == 0,
        "even": section % 2 == 0,
    }
    facts, masks, column, entering = lax.optimization_barrier((facts, masks, column, entering))

    def known(name, turn):
        if isinstance(turn, int):
            return facts[name][turn]
        if name == "at":
            return section == turn
        return jnp.clip((turn - section) // 2, 0, GROUPS - 1)

    def own_of(other, k=0):
        start = (facts["start"][k], jnp.zeros_like(facts["start"][k]))
        return lax.dynamic_slice(
            other, start, (rows, features), allow_negative_indices=False
        )

    arrived = [
        [entering[q]] + [jnp.zeros_like(entering[q])] * (chips - 1) for q in range(STREAMS)
    ]
    blank = jnp.zeros((rows, features), jnp.bfloat16)
    saved = [[blank] * GROUPS for _ in range(STREAMS)]
    final = [[blank] * GROUPS for _ in range(STREAMS)]

    def one_turn(turn, odd, state, ending=False):
        arrived, saved, final, behind = state
        arrived = [list(x) for x in arrived]
        saved, final = [list(x) for x in saved], [list(x) for x in final]
        for q in range(STREAMS):
            late = STREAMS - 1 - q
            if behind is not None:
                before = odd if q > 0 else not odd
                arrived[late] = []
                for k in range(chips):
                    arrived[late].append(to_paired(behind, before, 2 * k + 1))
                arrived[q] = list(lax.optimization_barrier((behind, *arrived[q])))[1:]
            mine = sum(a.astype(jnp.float32) for a in arrived[q]).astype(jnp.bfloat16)
            if not odd:
                for i in range(1, GROUPS):
                    fresh = facts["at"][0]
                    if not isinstance(turn, int):
                        fresh = jnp.logical_and(fresh, turn == 2 * i)
                    elif turn != 2 * i:
                        continue
                    mine = jnp.where(fresh, entering[i * STREAMS + q], mine)
            other = swapped(mine)
            own = own_of(other)
            for i in range(GROUPS):
                if not isinstance(turn, int):
                    ended = turn == sections + 2 * i
                    final[q][i] = jnp.where(ended, own, final[q][i])
                elif turn == sections + 2 * i:
                    final[q][i] = own
                if not isinstance(turn, int) or 1 <= turn - 2 * i < sections:
                    here = known("at", turn - 2 * i)
                    saved[q][i] = jnp.where(here, own, saved[q][i])
            index = known("index", turn)
            nought = jnp.zeros_like(index)
            mask = lax.dynamic_slice(
                masks[q], (index, nought, nought), (1,) + masks.shape[2:],
                allow_negative_indices=False,
            )[0]
            send, keep = run_expert(
                mine, other, mask, gain, column, expert_in, expert_out,
                mine if behind is None else behind,
            )
            came = swapped(send)
            stream = jnp.where(facts["lead"], other, jnp.zeros_like(other)).astype(jnp.float32)
            partial = keep.astype(jnp.float32) + came.astype(jnp.float32) + stream
            behind = partial.astype(jnp.bfloat16)
            if ending:
                own = own_of(partial)
                for k in range(1, chips):
                    own = own + across(
                        own_of(behind, k), lambda s, e, k=k: (s, e ^ (2 * k))
                    ).astype(jnp.float32)
                final[q][GROUPS - 1] = own.astype(jnp.bfloat16)
                if q == 0:
                    behind = None
        return arrived, saved, final, behind

    def two_turns(pair, state):
        return one_turn(2 * pair + 1, True, one_turn(2 * pair, False, state))

    state = two_turns(0, (arrived, saved, final, None))
    if sections * chips <= UNROLLED:
        for pair in range(1, turns // 2 - 1):
            state = two_turns(pair, state)
    else:
        state = lax.fori_loop(1, turns // 2 - 1, two_turns, state)
    state = one_turn(turns - 2, False, state)
    arrived, saved, final, _ = one_turn(turns - 1, True, state, ending=True)

    def whole(values):
        return jnp.stack([values[q][i] for i in range(GROUPS) for q in range(STREAMS)])

    passed = whole(saved).reshape(-1, features)
    from_even, from_odd = to_paired(passed, False, 0), to_paired(passed, True, 0)
    returned = jnp.where(facts["even"], from_even, from_odd)
    states = jnp.where(facts["at"][sections - 1], whole(final).reshape(-1, features), returned)
    return states.reshape(1, micro_count, tok_rows, features)


def solution(mesh):
    placed = (
        P(None, "expert", None),
        P("section", None, None, None),
        P("section", None, None),
        P("section", None),
        P("section", "expert", None, None),
        P("section", "expert", None, None),
    )
    return jax.shard_map(
        body,
        mesh=mesh,
        in_specs=placed,
        out_specs=P("section", None, "expert", None),
        check_vma=False,
    )
```

```python
import jax
import jax.numpy as jnp
from jax import lax
from jax.experimental import pallas as pl
from jax.experimental.pallas import tpu as pltpu
from jax.sharding import PartitionSpec as P


epsilon = 1e-06
STREAMS = 2
GROUPS = 2
LANES = 128
UNROLLED = 32


def expert_kernel(
    mine_ref, other_ref, mask_ref, gain_ref, router_ref, in_ref, out_ref, behind_ref,
    send_ref, keep_ref,
):
    half, features = mine_ref.shape
    block = min(half, 64)

    def group(g, carry):
        rows = pl.ds(pl.multiple_of(g * block, block), block)
        lower = pl.ds(pl.multiple_of(half + g * block, block), block)

        def normed_of(ref):
            stream = ref[rows, :].astype(jnp.float32)
            inverse = lax.rsqrt(jnp.mean(stream * stream, axis=-1, keepdims=True) + epsilon)
            return (stream * inverse * gain_ref[...]).astype(jnp.bfloat16)

        normed = jnp.concatenate([normed_of(mine_ref), normed_of(other_ref)], axis=0)
        logits = jnp.dot(normed, router_ref[...], preferred_element_type=jnp.float32)
        mask = jnp.concatenate([mask_ref[rows, :], mask_ref[lower, :]], axis=0)
        gate = jax.nn.sigmoid(logits) * mask
        hidden = jnp.dot(normed, in_ref[...], preferred_element_type=jnp.float32)
        hidden = jnp.maximum(hidden, 0.0).astype(jnp.bfloat16)
        total = jnp.dot(hidden, out_ref[...], preferred_element_type=jnp.float32)
        for column in range(0, features, LANES):
            lanes = slice(column, column + LANES)
            gated = (total[:, lanes] * gate).astype(send_ref.dtype)
            send_ref[rows, lanes] = gated[:block]
            keep_ref[rows, lanes] = gated[block:]
        return carry

    if half == block:
        group(0, 0)
    else:
        lax.fori_loop(0, half // block, group, 0)


def load_kernel(in_ref, out_ref, in_local, out_local, sems):
    pieces = sems.shape[1]
    copies = []
    for n, (source, target) in enumerate(((in_ref, in_local), (out_ref, out_local))):
        size = source.shape[0] // pieces
        for i in range(pieces):
            part = pl.ds(i * size, size)
            copies.append(
                pltpu.make_async_copy(source.at[part, :], target.at[part, :], sems.at[n, i])
            )
    for copy in copies:
        copy.start()
    for copy in copies:
        copy.wait()


def load(weight_in, weight_out):
    local = pl.BlockSpec(memory_space=pltpu.VMEM)
    return pl.pallas_call(
        load_kernel,
        out_shape=tuple(jax.ShapeDtypeStruct(w.shape, w.dtype) for w in (weight_in, weight_out)),
        in_specs=[pl.BlockSpec(memory_space=pltpu.HBM)] * 2,
        out_specs=(local,) * 2,
        scratch_shapes=[pltpu.SemaphoreType.DMA((2, 4))],
        compiler_params=pltpu.CompilerParams(vmem_limit_bytes=43 * 2**20),
        cost_estimate=pl.CostEstimate(
            flops=2 * weight_in.size * 1024, bytes_accessed=8 * weight_in.size, transcendentals=0
        ),
    )(weight_in, weight_out)


def run_expert(mine, other, mask, gain, router, weight_in, weight_out, behind):
    half, features = mine.shape
    hidden_total = weight_in.shape[1]
    local = pl.BlockSpec(memory_space=pltpu.VMEM)
    return pl.pallas_call(
        expert_kernel,
        out_shape=(jax.ShapeDtypeStruct(mine.shape, jnp.bfloat16),) * 2,
        in_specs=[local] * 7 + [pl.BlockSpec(memory_space=pl.ANY)],
        out_specs=(local,) * 2,
        compiler_params=pltpu.CompilerParams(vmem_limit_bytes=20 * 2**20),
        cost_estimate=pl.CostEstimate(
            flops=8 * half * features * hidden_total,
            bytes_accessed=4 * features * hidden_total,
            transcendentals=0,
        ),
    )(mine, other, mask, gain, router, weight_in, weight_out, behind)


def body(tokens, route_ids, router, norm_gain, weight_in, weight_out):
    sections, experts = lax.axis_size("section"), lax.axis_size("expert")
    section, member = lax.axis_index("section"), lax.axis_index("expert")
    chip, core = member // 2, member % 2
    chips = experts // 2
    micro_count, tok_rows, features = tokens.shape
    pieces = STREAMS * GROUPS
    part = micro_count // pieces
    rows = part * tok_rows
    gain = norm_gain.astype(jnp.float32)
    expert_in, expert_out = weight_in[0, 0], weight_out[0, 0]
    column = lax.dynamic_slice_in_dim(router[0], member, 1, axis=1)
    column = jnp.broadcast_to(column, (features, LANES))

    named = jnp.any(route_ids[0] == member, axis=-1)
    named = named.reshape(GROUPS, STREAMS, part, chips, 2, tok_rows).transpose(1, 0, 4, 3, 2, 5)
    named = jnp.where(core == 0, named[:, :, ::-1], named).astype(jnp.float32)
    masks = named.reshape(STREAMS, GROUPS, experts * rows, 1)
    masks = jnp.broadcast_to(masks, masks.shape[:3] + (LANES,))

    def place(s, e):
        return s * experts + e

    def across(value, other_of):
        pairs = [
            (place(s, e), place(*other_of(s, e))) for s in range(sections) for e in range(experts)
        ]
        return lax.ppermute(value, ("section", "expert"), pairs)

    def to_paired(value, odd, flip):
        def other_of(s, e):
            other = s - 1 if (s % 2 == 0) == odd else s + 1
            if 0 <= other < sections:
                return (other, e ^ flip)
            return (s, e ^ (flip or 1))

        return across(value, other_of)

    def swapped(value):
        return across(value, lambda s, e: (s, e ^ 1))

    def from_chips(value):
        return [across(value, lambda s, e, k=k: (s, e ^ (2 * k + 1))) for k in range(chips)]

    own_tokens = tokens.reshape(-1, features)
    first, later = from_chips(own_tokens[:rows]), from_chips(own_tokens[rows:])
    turns = sections + 2 * (GROUPS - 1)
    facts = {
        "at": [section == turn for turn in range(turns)],
        "index": [
            jnp.clip((turn - section) // 2, 0, GROUPS - 1).astype(jnp.int32)
            for turn in range(turns)
        ],
        "start": [(chip ^ k) * rows for k in range(chips)],
        "between": [[(chip ^ y) == k for k in range(chips)] for y in range(chips)],
        "lead": chip == 0,
        "even": section % 2 == 0,
    }
    facts, masks, column, expert_in, expert_out = lax.optimization_barrier(
        (facts, masks, column, expert_in, expert_out)
    )
    expert_in, expert_out = load(expert_in, expert_out)

    def by_chip(came, at):
        halves = []
        for y in range(chips):
            wanted = came[0]
            for k in range(1, chips):
                wanted = jnp.where(facts["between"][y][k], came[k], wanted)
            halves.append(wanted[at * rows : (at + 1) * rows])
        return jnp.concatenate(halves, axis=0)

    entering = [by_chip(first, 0)] + [by_chip(later, n) for n in range(pieces - 1)]

    def known(name, turn):
        if isinstance(turn, int):
            return facts[name][turn]
        if name == "at":
            return section == turn
        return jnp.clip((turn - section) // 2, 0, GROUPS - 1)

    def own_of(other, k=0):
        start = (facts["start"][k], jnp.zeros_like(facts["start"][k]))
        return lax.dynamic_slice(
            other, start, (rows, features), allow_negative_indices=False
        )

    arrived = [
        [entering[q]] + [jnp.zeros_like(entering[q])] * (chips - 1) for q in range(STREAMS)
    ]
    blank = jnp.zeros((rows, features), jnp.bfloat16)
    saved = [[blank] * GROUPS for _ in range(STREAMS)]
    final = [[blank] * GROUPS for _ in range(STREAMS)]

    def whole(values):
        return jnp.stack([values[q][i] for i in range(GROUPS) for q in range(STREAMS)])

    def one_turn(turn, odd, state, ending=False):
        arrived, saved, final, behind = state
        arrived = [list(x) for x in arrived]
        saved, final = [list(x) for x in saved], [list(x) for x in final]
        for q in range(STREAMS):
            late = STREAMS - 1 - q
            if behind is not None:
                before = odd if q > 0 else not odd
                arrived[late] = []
                for k in range(chips):
                    arrived[late].append(to_paired(behind, before, 2 * k + 1))
                arrived[q] = list(lax.optimization_barrier((behind, *arrived[q])))[1:]
            mine = sum(a.astype(jnp.float32) for a in arrived[q]).astype(jnp.bfloat16)
            if not odd:
                for i in range(1, GROUPS):
                    fresh = facts["at"][0]
                    if not isinstance(turn, int):
                        fresh = jnp.logical_and(fresh, turn == 2 * i)
                    elif turn != 2 * i:
                        continue
                    mine = jnp.where(fresh, entering[i * STREAMS + q], mine)
            other = swapped(mine)
            own = own_of(other)
            for i in range(GROUPS):
                if not isinstance(turn, int):
                    ended = turn == sections + 2 * i
                    final[q][i] = jnp.where(ended, own, final[q][i])
                elif turn == sections + 2 * i:
                    final[q][i] = own
                if not isinstance(turn, int) or 1 <= turn - 2 * i < sections:
                    here = known("at", turn - 2 * i)
                    saved[q][i] = jnp.where(here, own, saved[q][i])
            returned = None
            if ending and q == STREAMS - 1:
                passed = whole(saved).reshape(-1, features)
                from_even = to_paired(passed, False, 0)
                from_odd = to_paired(passed, True, 0)
                returned = jnp.where(facts["even"], from_even, from_odd)
            index = known("index", turn)
            nought = jnp.zeros_like(index)
            mask = lax.dynamic_slice(
                masks[q], (index, nought, nought), (1,) + masks.shape[2:],
                allow_negative_indices=False,
            )[0]
            send, keep = run_expert(
                mine, other, mask, gain, column, expert_in, expert_out,
                mine if behind is None else behind,
            )
            came = swapped(send)
            stream = jnp.where(facts["lead"], other, jnp.zeros_like(other)).astype(jnp.float32)
            partial = keep.astype(jnp.float32) + came.astype(jnp.float32) + stream
            behind = partial.astype(jnp.bfloat16)
            if ending:
                own = own_of(partial)
                for k in range(1, chips):
                    own = own + across(
                        own_of(behind, k), lambda s, e, k=k: (s, e ^ (2 * k))
                    ).astype(jnp.float32)
                final[q][GROUPS - 1] = own.astype(jnp.bfloat16)
                if q == 0:
                    behind = None
        if ending:
            return final, returned
        return arrived, saved, final, behind

    def two_turns(pair, state):
        return one_turn(2 * pair + 1, True, one_turn(2 * pair, False, state))

    state = two_turns(0, (arrived, saved, final, None))
    if sections * chips <= UNROLLED:
        for pair in range(1, turns // 2 - 1):
            state = two_turns(pair, state)
    else:
        state = lax.fori_loop(1, turns // 2 - 1, two_turns, state)
    state = one_turn(turns - 2, False, state)
    final, returned = one_turn(turns - 1, True, state, ending=True)

    states = jnp.where(facts["at"][sections - 1], whole(final).reshape(-1, features), returned)
    return states.reshape(1, micro_count, tok_rows, features)


def solution(mesh):
    placed = (
        P(None, "expert", None),
        P("section", None, None, None),
        P("section", None, None),
        P("section", None),
        P("section", "expert", None, None),
        P("section", "expert", None, None),
    )
    return jax.shard_map(
        body,
        mesh=mesh,
        in_specs=placed,
        out_specs=P("section", None, "expert", None),
        check_vma=False,
    )
```

```python
import functools

import jax
import jax.numpy as jnp
from jax import lax
from jax.experimental import pallas as pl
from jax.experimental.pallas import tpu as pltpu
from jax.sharding import PartitionSpec as P


epsilon = 1e-06
STREAMS = 2
GROUPS = 2
LANES = 128
UNROLLED = 32


def expert_kernel(
    parts, mine_ref, other_ref, mask_ref, gain_ref, router_ref, in_ref, out_ref, behind_ref,
    send_ref, keep_ref, total_ref,
):
    half, features = mine_ref.shape
    block = min(half, 64)

    def group(g, carry):
        rows = pl.ds(pl.multiple_of(g * block, block), block)
        lower = pl.ds(pl.multiple_of(half + g * block, block), block)

        def normed_of(ref):
            stream = ref[rows, :].astype(jnp.float32)
            inverse = lax.rsqrt(jnp.mean(stream * stream, axis=-1, keepdims=True) + epsilon)
            return (stream * inverse * gain_ref[...]).astype(jnp.bfloat16)

        normed = jnp.concatenate([normed_of(mine_ref), normed_of(other_ref)], axis=0)
        logits = jnp.dot(normed, router_ref[...], preferred_element_type=jnp.float32)
        mask = jnp.concatenate([mask_ref[rows, :], mask_ref[lower, :]], axis=0)
        gate = jax.nn.sigmoid(logits) * mask
        tile = in_ref.shape[1] // parts

        def product(i):
            some = pl.ds(pl.multiple_of(i * tile, tile), tile)
            hidden = jnp.dot(normed, in_ref[:, some], preferred_element_type=jnp.float32)
            hidden = jnp.maximum(hidden, 0.0).astype(jnp.bfloat16)
            return jnp.dot(hidden, out_ref[some, :], preferred_element_type=jnp.float32)

        if parts == 1:
            total = product(0)
        else:
            total_ref[...] = jnp.zeros_like(total_ref)

            def add(i, none):
                total_ref[...] += product(i)
                return none

            lax.fori_loop(0, parts, add, 0)
            total = total_ref[...]
        for column in range(0, features, LANES):
            lanes = slice(column, column + LANES)
            gated = (total[:, lanes] * gate).astype(send_ref.dtype)
            send_ref[rows, lanes] = gated[:block]
            keep_ref[rows, lanes] = gated[block:]
        return carry

    if half == block:
        group(0, 0)
    else:
        lax.fori_loop(0, half // block, group, 0)


def load_kernel(in_ref, out_ref, in_local, out_local, sems):
    pieces = sems.shape[1]
    copies = []
    for n, (source, target) in enumerate(((in_ref, in_local), (out_ref, out_local))):
        size = source.shape[0] // pieces
        for i in range(pieces):
            part = pl.ds(i * size, size)
            copies.append(
                pltpu.make_async_copy(source.at[part, :], target.at[part, :], sems.at[n, i])
            )
    for copy in copies:
        copy.start()
    for copy in copies:
        copy.wait()


def load(weight_in, weight_out):
    local = pl.BlockSpec(memory_space=pltpu.VMEM)
    return pl.pallas_call(
        load_kernel,
        out_shape=tuple(jax.ShapeDtypeStruct(w.shape, w.dtype) for w in (weight_in, weight_out)),
        in_specs=[pl.BlockSpec(memory_space=pltpu.HBM)] * 2,
        out_specs=(local,) * 2,
        scratch_shapes=[pltpu.SemaphoreType.DMA((2, 4))],
        compiler_params=pltpu.CompilerParams(vmem_limit_bytes=43 * 2**20),
        cost_estimate=pl.CostEstimate(
            flops=2 * weight_in.size * 1024, bytes_accessed=8 * weight_in.size, transcendentals=0
        ),
    )(weight_in, weight_out)


def run_expert(parts, mine, other, mask, gain, router, weight_in, weight_out, behind):
    half, features = mine.shape
    hidden_total = weight_in.shape[1]
    local = pl.BlockSpec(memory_space=pltpu.VMEM)
    return pl.pallas_call(
        functools.partial(expert_kernel, parts),
        out_shape=(jax.ShapeDtypeStruct(mine.shape, jnp.bfloat16),) * 2,
        in_specs=[local] * 7 + [pl.BlockSpec(memory_space=pl.ANY)],
        out_specs=(local,) * 2,
        scratch_shapes=[pltpu.VMEM((2 * min(half, 64), features), jnp.float32)],
        compiler_params=pltpu.CompilerParams(vmem_limit_bytes=20 * 2**20),
        cost_estimate=pl.CostEstimate(
            flops=8 * half * features * hidden_total,
            bytes_accessed=4 * features * hidden_total,
            transcendentals=0,
        ),
    )(mine, other, mask, gain, router, weight_in, weight_out, behind)


def body(tokens, route_ids, router, norm_gain, weight_in, weight_out):
    sections, experts = lax.axis_size("section"), lax.axis_size("expert")
    section, member = lax.axis_index("section"), lax.axis_index("expert")
    chip, core = member // 2, member % 2
    chips = experts // 2
    micro_count, tok_rows, features = tokens.shape
    pieces = STREAMS * GROUPS
    part = micro_count // pieces
    rows = part * tok_rows
    gain = norm_gain.astype(jnp.float32)
    expert_in, expert_out = weight_in[0, 0], weight_out[0, 0]
    column = lax.dynamic_slice_in_dim(router[0], member, 1, axis=1)
    column = jnp.broadcast_to(column, (features, LANES))

    named = jnp.any(route_ids[0] == member, axis=-1)
    named = named.reshape(GROUPS, STREAMS, part, chips, 2, tok_rows).transpose(1, 0, 4, 3, 2, 5)
    named = jnp.where(core == 0, named[:, :, ::-1], named).astype(jnp.float32)
    masks = named.reshape(STREAMS, GROUPS, experts * rows, 1)
    masks = jnp.broadcast_to(masks, masks.shape[:3] + (LANES,))

    def place(s, e):
        return s * experts + e

    def across(value, other_of):
        pairs = [
            (place(s, e), place(*other_of(s, e))) for s in range(sections) for e in range(experts)
        ]
        return lax.ppermute(value, ("section", "expert"), pairs)

    def to_paired(value, odd, flip):
        def other_of(s, e):
            other = s - 1 if (s % 2 == 0) == odd else s + 1
            if 0 <= other < sections:
                return (other, e ^ flip)
            return (s, e ^ (flip or 1))

        return across(value, other_of)

    def swapped(value):
        return across(value, lambda s, e: (s, e ^ 1))

    def from_chips(value):
        return [across(value, lambda s, e, k=k: (s, e ^ (2 * k + 1))) for k in range(chips)]

    own_tokens = tokens.reshape(-1, features)
    first, later = from_chips(own_tokens[:rows]), from_chips(own_tokens[rows:])
    turns = sections + 2 * (GROUPS - 1)
    facts = {
        "at": [section == turn for turn in range(turns)],
        "index": [
            jnp.clip((turn - section) // 2, 0, GROUPS - 1).astype(jnp.int32)
            for turn in range(turns)
        ],
        "start": [(chip ^ k) * rows for k in range(chips)],
        "between": [[(chip ^ y) == k for k in range(chips)] for y in range(chips)],
        "lead": chip == 0,
        "even": section % 2 == 0,
    }
    facts, masks, column, expert_in, expert_out = lax.optimization_barrier(
        (facts, masks, column, expert_in, expert_out)
    )
    expert_in, expert_out = load(expert_in, expert_out)

    def by_chip(came, at):
        halves = []
        for y in range(chips):
            wanted = came[0]
            for k in range(1, chips):
                wanted = jnp.where(facts["between"][y][k], came[k], wanted)
            halves.append(wanted[at * rows : (at + 1) * rows])
        return jnp.concatenate(halves, axis=0)

    entering = [by_chip(first, 0)] + [by_chip(later, n) for n in range(pieces - 1)]

    def known(name, turn):
        if isinstance(turn, int):
            return facts[name][turn]
        if name == "at":
            return section == turn
        return jnp.clip((turn - section) // 2, 0, GROUPS - 1)

    def own_of(other, k=0):
        start = (facts["start"][k], jnp.zeros_like(facts["start"][k]))
        return lax.dynamic_slice(
            other, start, (rows, features), allow_negative_indices=False
        )

    arrived = [
        [entering[q]] + [jnp.zeros_like(entering[q])] * (chips - 1) for q in range(STREAMS)
    ]
    blank = jnp.zeros((rows, features), jnp.bfloat16)
    saved = [[blank] * GROUPS for _ in range(STREAMS)]
    final = [[blank] * GROUPS for _ in range(STREAMS)]

    def whole(values):
        return jnp.stack([values[q][i] for i in range(GROUPS) for q in range(STREAMS)])

    def one_turn(turn, odd, state, ending=False):
        arrived, saved, final, behind = state
        arrived = [list(x) for x in arrived]
        saved, final = [list(x) for x in saved], [list(x) for x in final]
        for q in range(STREAMS):
            late = STREAMS - 1 - q
            if behind is not None:
                before = odd if q > 0 else not odd
                arrived[late] = []
                for k in range(chips):
                    arrived[late].append(to_paired(behind, before, 2 * k + 1))
                arrived[q] = list(lax.optimization_barrier((behind, *arrived[q])))[1:]
            mine = sum(a.astype(jnp.float32) for a in arrived[q]).astype(jnp.bfloat16)
            if not odd:
                for i in range(1, GROUPS):
                    fresh = facts["at"][0]
                    if not isinstance(turn, int):
                        fresh = jnp.logical_and(fresh, turn == 2 * i)
                    elif turn != 2 * i:
                        continue
                    mine = jnp.where(fresh, entering[i * STREAMS + q], mine)
            other = swapped(mine)
            own = own_of(other)
            for i in range(GROUPS):
                if not isinstance(turn, int):
                    ended = turn == sections + 2 * i
                    final[q][i] = jnp.where(ended, own, final[q][i])
                elif turn == sections + 2 * i:
                    final[q][i] = own
                if not isinstance(turn, int) or 1 <= turn - 2 * i < sections:
                    here = known("at", turn - 2 * i)
                    saved[q][i] = jnp.where(here, own, saved[q][i])
            returned = None
            if ending and q == STREAMS - 1:
                passed = whole(saved).reshape(-1, features)
                from_even = to_paired(passed, False, 0)
                from_odd = to_paired(passed, True, 0)
                returned = jnp.where(facts["even"], from_even, from_odd)
            index = known("index", turn)
            nought = jnp.zeros_like(index)
            mask = lax.dynamic_slice(
                masks[q], (index, nought, nought), (1,) + masks.shape[2:],
                allow_negative_indices=False,
            )[0]
            send, keep = run_expert(
                2 if odd == (q > 0) else 1, mine, other, mask, gain, column, expert_in, expert_out,
                mine if behind is None else behind,
            )
            came = swapped(send)
            stream = jnp.where(facts["lead"], other, jnp.zeros_like(other)).astype(jnp.float32)
            partial = keep.astype(jnp.float32) + came.astype(jnp.float32) + stream
            behind = partial.astype(jnp.bfloat16)
            if ending:
                own = own_of(partial)
                for k in range(1, chips):
                    own = own + across(
                        own_of(behind, k), lambda s, e, k=k: (s, e ^ (2 * k))
                    ).astype(jnp.float32)
                final[q][GROUPS - 1] = own.astype(jnp.bfloat16)
                if q == 0:
                    behind = None
        if ending:
            return final, returned
        return arrived, saved, final, behind

    def two_turns(pair, state):
        return one_turn(2 * pair + 1, True, one_turn(2 * pair, False, state))

    state = two_turns(0, (arrived, saved, final, None))
    if sections * chips <= UNROLLED:
        for pair in range(1, turns // 2 - 1):
            state = two_turns(pair, state)
    else:
        state = lax.fori_loop(1, turns // 2 - 1, two_turns, state)
    state = one_turn(turns - 2, False, state)
    final, returned = one_turn(turns - 1, True, state, ending=True)

    states = jnp.where(facts["at"][sections - 1], whole(final).reshape(-1, features), returned)
    return states.reshape(1, micro_count, tok_rows, features)


def solution(mesh):
    placed = (
        P(None, "expert", None),
        P("section", None, None, None),
        P("section", None, None),
        P("section", None),
        P("section", "expert", None, None),
        P("section", "expert", None, None),
    )
    return jax.shard_map(
        body,
        mesh=mesh,
        in_specs=placed,
        out_specs=P("section", None, "expert", None),
        check_vma=False,
    )
```

```python
import functools

import jax
import jax.numpy as jnp
from jax import lax
from jax.experimental import pallas as pl
from jax.experimental.pallas import tpu as pltpu
from jax.sharding import PartitionSpec as P


epsilon = 1e-06
STREAMS = 2
GROUPS = 2
LANES = 128
UNROLLED = 32


def expert_kernel(
    parts, mine_ref, other_ref, mask_ref, gain_ref, router_ref, in_ref, out_ref, behind_ref,
    send_ref, keep_ref, total_ref,
):
    half, features = mine_ref.shape
    block = min(half, 64)

    def group(g, carry):
        rows = pl.ds(pl.multiple_of(g * block, block), block)
        lower = pl.ds(pl.multiple_of(half + g * block, block), block)

        def normed_of(ref):
            stream = ref[rows, :].astype(jnp.float32)
            inverse = lax.rsqrt(jnp.mean(stream * stream, axis=-1, keepdims=True) + epsilon)
            return (stream * inverse * gain_ref[...]).astype(jnp.bfloat16)

        normed = jnp.concatenate([normed_of(mine_ref), normed_of(other_ref)], axis=0)
        logits = jnp.dot(normed, router_ref[...], preferred_element_type=jnp.float32)
        mask = jnp.concatenate([mask_ref[rows, :], mask_ref[lower, :]], axis=0)
        gate = jax.nn.sigmoid(logits) * mask
        tile = in_ref.shape[1] // parts

        def product(i):
            some = pl.ds(pl.multiple_of(i * tile, tile), tile)
            hidden = jnp.dot(normed, in_ref[:, some], preferred_element_type=jnp.float32)
            hidden = jnp.maximum(hidden, 0.0).astype(jnp.bfloat16)
            return jnp.dot(hidden, out_ref[some, :], preferred_element_type=jnp.float32)

        if parts == 1:
            total = product(0)
        else:
            total_ref[...] = jnp.zeros_like(total_ref)

            def add(i, none):
                total_ref[...] += product(i)
                return none

            lax.fori_loop(0, parts, add, 0)
            total = total_ref[...]
        for column in range(0, features, LANES):
            lanes = slice(column, column + LANES)
            gated = (total[:, lanes] * gate).astype(send_ref.dtype)
            send_ref[rows, lanes] = gated[:block]
            keep_ref[rows, lanes] = gated[block:]
        return carry

    if half == block:
        group(0, 0)
    else:
        lax.fori_loop(0, half // block, group, 0)


def load_kernel(in_ref, out_ref, in_local, out_local, sems):
    pieces = sems.shape[1]
    copies = []
    for n, (source, target) in enumerate(((in_ref, in_local), (out_ref, out_local))):
        size = source.shape[0] // pieces
        for i in range(pieces):
            part = pl.ds(i * size, size)
            copies.append(
                pltpu.make_async_copy(source.at[part, :], target.at[part, :], sems.at[n, i])
            )
    for copy in copies:
        copy.start()
    for copy in copies:
        copy.wait()


def load(weight_in, weight_out):
    local = pl.BlockSpec(memory_space=pltpu.VMEM)
    return pl.pallas_call(
        load_kernel,
        out_shape=tuple(jax.ShapeDtypeStruct(w.shape, w.dtype) for w in (weight_in, weight_out)),
        in_specs=[pl.BlockSpec(memory_space=pltpu.HBM)] * 2,
        out_specs=(local,) * 2,
        scratch_shapes=[pltpu.SemaphoreType.DMA((2, 4))],
        compiler_params=pltpu.CompilerParams(vmem_limit_bytes=43 * 2**20),
        cost_estimate=pl.CostEstimate(
            flops=2 * weight_in.size * 1024, bytes_accessed=8 * weight_in.size, transcendentals=0
        ),
    )(weight_in, weight_out)


def run_expert(parts, mine, other, mask, gain, router, weight_in, weight_out, behind):
    half, features = mine.shape
    hidden_total = weight_in.shape[1]
    local = pl.BlockSpec(memory_space=pltpu.VMEM)
    return pl.pallas_call(
        functools.partial(expert_kernel, parts),
        out_shape=(jax.ShapeDtypeStruct(mine.shape, jnp.bfloat16),) * 2,
        in_specs=[local] * 7 + [pl.BlockSpec(memory_space=pl.ANY)],
        out_specs=(local,) * 2,
        scratch_shapes=[pltpu.VMEM((2 * min(half, 64), features), jnp.float32)],
        compiler_params=pltpu.CompilerParams(vmem_limit_bytes=20 * 2**20),
        cost_estimate=pl.CostEstimate(
            flops=8 * half * features * hidden_total,
            bytes_accessed=4 * features * hidden_total,
            transcendentals=0,
        ),
    )(mine, other, mask, gain, router, weight_in, weight_out, behind)


def body(tokens, route_ids, router, norm_gain, weight_in, weight_out):
    sections, experts = lax.axis_size("section"), lax.axis_size("expert")
    section, member = lax.axis_index("section"), lax.axis_index("expert")
    chip, core = member // 2, member % 2
    chips = experts // 2
    micro_count, tok_rows, features = tokens.shape
    pieces = STREAMS * GROUPS
    part = micro_count // pieces
    rows = part * tok_rows
    gain = norm_gain.astype(jnp.float32)
    expert_in, expert_out = weight_in[0, 0], weight_out[0, 0]
    column = lax.dynamic_slice_in_dim(router[0], member, 1, axis=1)
    column = jnp.broadcast_to(column, (features, LANES))

    named = jnp.any(route_ids[0] == member, axis=-1)
    named = named.reshape(GROUPS, STREAMS, part, chips, 2, tok_rows).transpose(1, 0, 4, 3, 2, 5)
    named = jnp.where(core == 0, named[:, :, ::-1], named).astype(jnp.float32)
    masks = named.reshape(STREAMS, GROUPS, experts * rows, 1)
    masks = jnp.broadcast_to(masks, masks.shape[:3] + (LANES,))

    def place(s, e):
        return s * experts + e

    def across(value, other_of):
        pairs = [
            (place(s, e), place(*other_of(s, e))) for s in range(sections) for e in range(experts)
        ]
        return lax.ppermute(value, ("section", "expert"), pairs)

    def to_paired(value, odd, flip):
        def other_of(s, e):
            other = s - 1 if (s % 2 == 0) == odd else s + 1
            if 0 <= other < sections:
                return (other, e ^ flip)
            return (s, e ^ (flip or 1))

        return across(value, other_of)

    def swapped(value):
        return across(value, lambda s, e: (s, e ^ 1))

    def from_chips(value):
        return [across(value, lambda s, e, k=k: (s, e ^ (2 * k + 1))) for k in range(chips)]

    own_tokens = tokens.reshape(-1, features)
    first, later = from_chips(own_tokens[:rows]), from_chips(own_tokens[rows:])
    turns = sections + 2 * (GROUPS - 1)
    facts = {
        "at": [section == turn for turn in range(turns)],
        "index": [
            jnp.clip((turn - section) // 2, 0, GROUPS - 1).astype(jnp.int32)
            for turn in range(turns)
        ],
        "start": [(chip ^ k) * rows for k in range(chips)],
        "between": [[(chip ^ y) == k for k in range(chips)] for y in range(chips)],
        "lead": chip == 0,
        "even": section % 2 == 0,
    }
    facts, masks, column, expert_in, expert_out = lax.optimization_barrier(
        (facts, masks, column, expert_in, expert_out)
    )
    expert_in, expert_out = load(expert_in, expert_out)

    def by_chip(came, at):
        halves = []
        for y in range(chips):
            wanted = came[0]
            for k in range(1, chips):
                wanted = jnp.where(facts["between"][y][k], came[k], wanted)
            halves.append(wanted[at * rows : (at + 1) * rows])
        return jnp.concatenate(halves, axis=0)

    entering = [by_chip(first, 0)] + [by_chip(later, n) for n in range(pieces - 1)]

    def known(name, turn):
        if isinstance(turn, int):
            return facts[name][turn]
        if name == "at":
            return section == turn
        return jnp.clip((turn - section) // 2, 0, GROUPS - 1)

    def own_of(other, k=0):
        start = (facts["start"][k], jnp.zeros_like(facts["start"][k]))
        return lax.dynamic_slice(
            other, start, (rows, features), allow_negative_indices=False
        )

    arrived = [
        [entering[q]] + [jnp.zeros_like(entering[q])] * (chips - 1) for q in range(STREAMS)
    ]
    blank = jnp.zeros((rows, features), jnp.bfloat16)
    saved = [[blank] * GROUPS for _ in range(STREAMS)]
    final = [[blank] * GROUPS for _ in range(STREAMS)]

    def whole(values):
        return jnp.stack([values[q][i] for i in range(GROUPS) for q in range(STREAMS)])

    def one_turn(turn, odd, state, ending=False):
        arrived, saved, final, behind = state
        arrived = [list(x) for x in arrived]
        saved, final = [list(x) for x in saved], [list(x) for x in final]
        for q in range(STREAMS):
            late = STREAMS - 1 - q
            if behind is not None:
                before = odd if q > 0 else not odd
                arrived[late] = []
                for k in range(chips):
                    flip = 2 * (chips - 1 - k) + 1
                    arrived[late].append(to_paired(behind, before, flip))
                arrived[q] = list(lax.optimization_barrier((behind, *arrived[q])))[1:]
            mine = sum(a.astype(jnp.float32) for a in arrived[q]).astype(jnp.bfloat16)
            if not odd:
                for i in range(1, GROUPS):
                    fresh = facts["at"][0]
                    if not isinstance(turn, int):
                        fresh = jnp.logical_and(fresh, turn == 2 * i)
                    elif turn != 2 * i:
                        continue
                    mine = jnp.where(fresh, entering[i * STREAMS + q], mine)
            other = swapped(mine)
            own = own_of(other)
            for i in range(GROUPS):
                if not isinstance(turn, int):
                    ended = turn == sections + 2 * i
                    final[q][i] = jnp.where(ended, own, final[q][i])
                elif turn == sections + 2 * i:
                    final[q][i] = own
                if not isinstance(turn, int) or 1 <= turn - 2 * i < sections:
                    here = known("at", turn - 2 * i)
                    saved[q][i] = jnp.where(here, own, saved[q][i])
            returned = None
            if ending and q == STREAMS - 1:
                passed = whole(saved).reshape(-1, features)
                from_even = to_paired(passed, False, 0)
                from_odd = to_paired(passed, True, 0)
                returned = jnp.where(facts["even"], from_even, from_odd)
            index = known("index", turn)
            nought = jnp.zeros_like(index)
            mask = lax.dynamic_slice(
                masks[q], (index, nought, nought), (1,) + masks.shape[2:],
                allow_negative_indices=False,
            )[0]
            edge = ending or (isinstance(turn, int) and turn == 0)
            parts = 2 if odd == (q > 0) and not edge else 1
            send, keep = run_expert(
                parts, mine, other, mask, gain, column, expert_in, expert_out,
                mine if behind is None else behind,
            )
            came = swapped(send)
            stream = jnp.where(facts["lead"], other, jnp.zeros_like(other)).astype(jnp.float32)
            partial = keep.astype(jnp.float32) + came.astype(jnp.float32) + stream
            behind = partial.astype(jnp.bfloat16)
            if ending:
                own = own_of(partial)
                for k in range(1, chips):
                    own = own + across(
                        own_of(behind, k), lambda s, e, k=k: (s, e ^ (2 * k))
                    ).astype(jnp.float32)
                final[q][GROUPS - 1] = own.astype(jnp.bfloat16)
                if q == 0:
                    behind = None
        if ending:
            return final, returned
        return arrived, saved, final, behind

    def two_turns(pair, state):
        return one_turn(2 * pair + 1, True, one_turn(2 * pair, False, state))

    state = two_turns(0, (arrived, saved, final, None))
    if sections * chips <= UNROLLED:
        for pair in range(1, turns // 2 - 1):
            state = two_turns(pair, state)
    else:
        state = lax.fori_loop(1, turns // 2 - 1, two_turns, state)
    state = one_turn(turns - 2, False, state)
    final, returned = one_turn(turns - 1, True, state, ending=True)

    states = jnp.where(facts["at"][sections - 1], whole(final).reshape(-1, features), returned)
    return states.reshape(1, micro_count, tok_rows, features)


def solution(mesh):
    placed = (
        P(None, "expert", None),
        P("section", None, None, None),
        P("section", None, None),
        P("section", None),
        P("section", "expert", None, None),
        P("section", "expert", None, None),
    )
    return jax.shard_map(
        body,
        mesh=mesh,
        in_specs=placed,
        out_specs=P("section", None, "expert", None),
        check_vma=False,
    )
```
